32 devices in a mesh: row: 2 (over core), sector: 4 (over z), slab: 4 (over y, x).
Axes of the slice: x: 2, y: 2, z: 4, core: 2. Of those that a mesh axis runs over, the one named last changes fastest.
Arguments:
- state: float32 [2, 5, 32, 128, 128], P('row', None, 'slab', 'sector'), may hold values from -6 to 6
- source: float32 [2, 5, 32, 128, 128], P('row', None, 'slab', 'sector'), may hold values from -6 to 6
- diag_inverse: float32 [2, 5, 5, 32, 128, 128], P('row', None, None, 'slab', 'sector'), may hold values from -1 to 1
- jac_axial: float32 [2, 5, 5], P('row'), may hold values from -1 to 2
- jac_cross: float32 [2, 2, 5, 5], P('row'), may hold values from -2.5 to 2.5
- owner: int32 [128], replicated, may hold values from 0 to 127, as said below
Outputs:
- residual: float32 [2, 5, 32, 128, 128], P('row', None, 'slab', 'sector')
- new_state: float32 [2, 5, 32, 128, 128], P('row', None, 'slab', 'sector')
The draws below stay inside these ranges and needn't reach their ends.
Inputs may be any that keep to these rules, and one draw needn't show every extreme that they name: owner is a permutation; for some whole s, the columns b * 32 to b * 32 + 31 of the rotor face exactly the stator columns s + b * 32 to s + b * 32 + 31, taken modulo 128, for every b.
All inputs are finite; a program needn't handle non-finite values.
Results may differ from the reference program's by a relative error of at most 0.0001.
Values sent between devices are 32-bit elements; how exact they have to be, the bound alone decides.
A program may use at most 64 MiB of HBM per device.

```python
import jax
import jax.numpy as jnp
from jax import lax

VARS = 5
C = 32
R = 128
AXIAL_PLANES = 32
NC = 128


def draw_diag_inverse(key, part):
    first, second, third, fourth = jax.random.split(jax.random.fold_in(key, 11), 4)
    doubling_level = jax.random.uniform(first, (2, AXIAL_PLANES, NC, R), jnp.float32, 0.92, 1.0)
    plane_positions = jax.random.randint(second, (2, 3), 0, AXIAL_PLANES)
    sweep_group = jnp.any(jnp.arange(AXIAL_PLANES)[None, :, None] == plane_positions[:, None, :], axis=2)
    doubling_level = doubling_level * jnp.where(sweep_group, 0.6, 1.0)[:, :, None, None]
    vary = jax.random.uniform(fourth, (2, 5, AXIAL_PLANES, NC, R), jnp.float32, 0.85, 1.0)
    diagonal = doubling_level[:, None] * vary
    noise = 0.06 * jax.random.normal(third, (2, 5, 5, AXIAL_PLANES, NC, R), jnp.float32)
    identity = jnp.eye(5, dtype=jnp.float32)[None, :, :, None, None, None]
    return identity * diagonal[:, :, None] + (1.0 - identity) * noise


def draw_jac_axial(key, part):
    first, second = jax.random.split(jax.random.fold_in(key, 17), 2)
    rates = jax.random.uniform(first, (2, 5), jnp.float32, 0.9, 0.98)
    noise = 0.08 * jax.random.normal(second, (2, 5, 5), jnp.float32)
    identity = jnp.eye(5, dtype=jnp.float32)[None]
    return identity * (2.0 * rates)[:, :, None] + (1.0 - identity) * noise


def draw_owner(key, part):
    first, second = jax.random.split(jax.random.fold_in(key, 23), 2)
    offset = jax.random.randint(first, (), 0, NC)
    blocks = NC // C
    scores = jax.random.randint(second, (blocks, C), 0, 2 ** 20) * C + jnp.arange(C, dtype=jnp.int32)[None, :]
    within = jnp.argsort(scores, axis=1).astype(jnp.int32)
    starts = jnp.arange(blocks, dtype=jnp.int32)[:, None] * C
    return ((offset + starts + within) % NC).reshape(NC).astype(jnp.int32)


def steps_of(own_key, dims, cuts, smallest, high):
    def one(dim, blocks):
        draws = jax.random.uniform(jax.random.fold_in(jax.random.fold_in(own_key, 6), dim), (blocks,), jnp.float32, smallest / len(cuts), high / len(cuts))
        return jnp.repeat(jnp.exp(draws), dims[dim] // blocks).reshape((-1,) + (1,) * (len(dims) - dim - 1))

    loudness = one(*cuts[0])
    for cut in cuts[1:]:
        loudness = loudness * one(*cut)
    return loudness


def normal_values(stream_key, dims, scale, limit, pieces=(), kind=jnp.bfloat16):
    factor_of = steps_of(stream_key, dims, pieces, -0.22, 0.18) if pieces else 1.0
    entries = jax.random.normal(stream_key, dims, jnp.float32) * scale * factor_of
    return jnp.minimum(jnp.maximum(entries, -limit), limit).astype(kind)


def setup_inputs(seed: int = 0) -> dict:
    seeds = jax.random.split(jax.random.key(seed), 7)
    return {
        "state": normal_values(seeds[0], (2, VARS, AXIAL_PLANES, NC, R), 1.0, 6.0, ((0, 2), (2, 4), (3, 4)), jnp.float32),
        "source": normal_values(seeds[1], (2, VARS, AXIAL_PLANES, NC, R), 1.0, 6.0, ((0, 2), (2, 4), (3, 4)), jnp.float32),
        "diag_inverse": draw_diag_inverse(jax.random.fold_in(seeds[6], 71), 0),
        "jac_axial": draw_jac_axial(jax.random.fold_in(seeds[6], 71), 0),
        "jac_cross": normal_values(seeds[4], (2, 2, VARS, VARS), VARS ** -0.5, 2.5, ((0, 2),), jnp.float32),
        "owner": draw_owner(jax.random.fold_in(seeds[6], 71), 0),
    }


exact_mode = lax.Precision.HIGHEST


def mix_const(matrix, field):
    return jnp.einsum('ij,j...->i...', matrix, field, precision=exact_mode)


def per_cell(blocks, field):
    return jnp.sum(blocks * field[None], axis=1)


def forward_sweep(residual, inverse, axial, entering):
    planes = residual.shape[1]

    def advance(plane_at, carried):
        previous, output = carried
        block = lax.dynamic_index_in_dim(inverse, plane_at, 2, keepdims=False)
        value = lax.dynamic_index_in_dim(residual, plane_at, 1, keepdims=False)
        present_plane = per_cell(block, value + 0.5 * mix_const(axial, previous))
        output = lax.dynamic_update_index_in_dim(output, present_plane, plane_at, 1)
        return present_plane, output

    final_plane, output = lax.fori_loop(0, planes, advance, (entering, jnp.zeros_like(residual)))
    return output


def backward_sweep(provisional, inverse, axial, entering):
    planes = provisional.shape[1]

    def advance(step_at, carried):
        following, output = carried
        plane_at = planes - 1 - step_at
        block = lax.dynamic_index_in_dim(inverse, plane_at, 2, keepdims=False)
        value = lax.dynamic_index_in_dim(provisional, plane_at, 1, keepdims=False)
        present_plane = value - per_cell(block, 0.5 * mix_const(axial, following))
        output = lax.dynamic_update_index_in_dim(output, present_plane, plane_at, 1)
        return present_plane, output

    final_plane, output = lax.fori_loop(0, planes, advance, (entering, jnp.zeros_like(provisional)))
    return output


def flux_residual(field, source, axial, circular, radial_jac, below, above):
    axial_padded = jnp.concatenate([below[:, None], field, above[:, None]], axis=1)
    axial_diff = axial_padded[:, 2:] - axial_padded[:, :-2]
    cycle_diff = jnp.roll(field, -1, axis=2) - jnp.roll(field, 1, axis=2)
    radial = jnp.pad(field, ((0, 0), (0, 0), (0, 0), (1, 1)))
    radial_diff = radial[..., 2:] - radial[..., :-2]
    return source - 0.5 * (mix_const(axial, axial_diff) + mix_const(circular, cycle_diff) + mix_const(radial_jac, radial_diff))


def reference(state, source, diag_inverse, jac_axial, jac_cross, owner):
    zeros_plane = jnp.zeros_like(state[0][:, 0])
    rotor_above = jnp.take(state[1][:, 0], owner, axis=1)
    stator_below = zeros_plane.at[:, owner].set(state[0][:, -1])
    bounds = ((zeros_plane, rotor_above), (stator_below, zeros_plane))
    residuals = []
    updated = []
    for blade_row in range(2):
        field = state[blade_row]
        residual = flux_residual(field, source[blade_row], jac_axial[blade_row], jac_cross[blade_row, 0], jac_cross[blade_row, 1], bounds[blade_row][0], bounds[blade_row][1])
        provisional = forward_sweep(residual, diag_inverse[blade_row], jac_axial[blade_row], zeros_plane)
        update = backward_sweep(provisional, diag_inverse[blade_row], jac_axial[blade_row], zeros_plane)
        residuals.append(residual)
        updated.append(field + update)
    return jnp.stack(residuals), jnp.stack(updated)
```

```python
import functools

import jax
import jax.numpy as jnp
from jax import lax
from jax.experimental import pallas as pl
from jax.experimental.pallas import tpu as pltpu
from jax.sharding import PartitionSpec as P

MESH = pl.DeviceIdType.MESH
PAD = 8
GROUP = 8


def total(terms):
    while len(terms) > 1:
        pairs = [a + b for a, b in zip(terms[::2], terms[1::2])]
        if len(terms) % 2:
            pairs.append(terms[-1])
        terms = pairs
    return terms[0]


def kernel(
    sectors, slabs,
    state, source, inverse, axial, cross, picks,
    residual_out, state_out,
    q, src, inv, eff, res, prov, upd, facing, entering, following,
    local_sem, out_sem, ax_send, ax_recv, se_send, se_recv,
    if_send, if_recv, fw_send, fw_recv, bw_send, bw_recv,
):
    nv, planes, columns, cells = src.shape
    groups = columns // GROUP
    row = lax.axis_index("row")
    sector = lax.axis_index("sector")
    slab = lax.axis_index("slab")
    has_low = slab > 0
    has_high = slab < slabs - 1
    rotor_top = jnp.logical_and(row == 0, slab == slabs - 1)
    stator_foot = jnp.logical_and(row == 1, slab == 0)
    on_plane = jnp.logical_or(rotor_top, stator_foot)
    after = lax.rem(sector + 1, sectors)
    before = lax.rem(sector + sectors - 1, sectors)
    facing_slab = jnp.where(row == 0, 0, slabs - 1)
    body = pl.ds(PAD, columns)

    load_state = pltpu.make_async_copy(
        state.at[0], q.at[:, pl.ds(1, planes), body], local_sem.at[0]
    )
    load_state.start()
    load_inverse = pltpu.make_async_copy(inverse.at[0], inv, local_sem.at[2])
    load_inverse.start()
    load_source = pltpu.make_async_copy(source.at[0], src, local_sem.at[1])
    load_source.start()

    barrier = pltpu.get_barrier_semaphore()

    def greet(**where):
        pl.semaphore_signal(barrier, inc=1, device_id=where, device_id_type=MESH)

    @pl.when(on_plane)
    def _():
        for other in range(sectors):
            greet(row=1 - row, sector=other, slab=facing_slab)

    greet(sector=after)
    greet(sector=before)

    @pl.when(has_low)
    def _():
        greet(slab=slab - 1)

    @pl.when(has_high)
    def _():
        greet(slab=slab + 1)

    zero_plane = jnp.zeros((nv, columns, cells), jnp.float32)

    @pl.when(jnp.logical_not(has_low))
    def _():
        q[:, 0, body] = zero_plane

    @pl.when(jnp.logical_not(has_high))
    def _():
        q[:, planes + 1, body] = zero_plane

    peers = 2 + has_low.astype(jnp.int32) + has_high.astype(jnp.int32)
    pl.semaphore_wait(barrier, peers + jnp.where(on_plane, sectors, 0))

    load_state.wait()

    def remote(source_ref, target_ref, send, recv, **where):
        return pltpu.make_async_remote_copy(
            src_ref=source_ref, dst_ref=target_ref, send_sem=send, recv_sem=recv,
            device_id=where, device_id_type=MESH,
        )

    def facing_copy(plane_at, other):
        return remote(
            q.at[:, plane_at, body], facing.at[sector], if_send.at[other], if_recv.at[sector],
            row=1 - row, sector=other, slab=facing_slab,
        )

    def facing_arrival(other):
        return remote(
            q.at[:, 1, body], facing.at[other], if_send.at[other], if_recv.at[other],
            row=1 - row, sector=other, slab=facing_slab,
        )

    @pl.when(rotor_top)
    def _():
        for other in range(sectors):
            facing_copy(planes, other).start()

    @pl.when(stator_foot)
    def _():
        for other in range(sectors):
            facing_copy(1, other).start()

    inner = pl.ds(1, planes)
    to_after = remote(
        q.at[:, inner, pl.ds(PAD + columns - 1, 1)], q.at[:, inner, pl.ds(PAD - 1, 1)],
        se_send.at[0], se_recv.at[0], sector=after,
    )
    to_before = remote(
        q.at[:, inner, pl.ds(PAD, 1)], q.at[:, inner, pl.ds(PAD + columns, 1)],
        se_send.at[1], se_recv.at[1], sector=before,
    )
    to_after.start()
    to_before.start()
    to_high = remote(
        q.at[:, planes, body], q.at[:, 0, body], ax_send.at[0], ax_recv.at[0], slab=slab + 1
    )
    to_low = remote(
        q.at[:, 1, body], q.at[:, planes + 1, body], ax_send.at[1], ax_recv.at[1], slab=slab - 1
    )

    @pl.when(has_high)
    def _():
        to_high.start()

    @pl.when(has_low)
    def _():
        to_low.start()

    load_inverse.wait()

    def effective(x, carry):
        for i in range(nv):
            blocks = [inv[i, j, x] for j in range(nv)]
            for k in range(nv):
                eff[i, k, x] = total([blocks[j] * (0.5 * axial[0, j, k]) for j in range(nv)])
        return carry

    lax.fori_loop(0, planes, effective, 0)
    load_source.wait()
    to_after.wait_recv()
    to_before.wait_recv()

    @pl.when(has_high)
    def _():
        to_low.wait_recv()

    @pl.when(has_low)
    def _():
        to_high.wait_recv()

    def gather_facing(target):
        for other in range(sectors):
            facing_arrival(other).wait_recv()

        def pick(c, carry):
            at = picks[c]
            part, column = at // columns, lax.rem(at, columns)
            for v in range(nv):
                target[v, pl.ds(c, 1)] = facing[part, v, pl.ds(column, 1)]
            return carry

        lax.fori_loop(0, columns, pick, 0)

    @pl.when(rotor_top)
    def _():
        gather_facing(q.at[:, planes + 1, body])

    lane = lax.broadcasted_iota(jnp.int32, (columns, cells), 1)

    def flux(x, carry):
        sums = [None] * nv
        for v in range(nv):
            here = q[v, x + 1, body]
            spans = (
                q[v, x + 2, body] - q[v, x, body],
                q[v, x + 1, pl.ds(PAD + 1, columns)] - q[v, x + 1, pl.ds(PAD - 1, columns)],
                jnp.where(lane == cells - 1, 0.0, pltpu.roll(here, cells - 1, 1))
                - jnp.where(lane == 0, 0.0, pltpu.roll(here, 1, 1)),
            )
            for i in range(nv):
                factors = (axial[0, i, v], cross[0, 0, i, v], cross[0, 1, i, v])
                term = total([(0.5 * f) * s for f, s in zip(factors, spans)])
                sums[i] = term if sums[i] is None else sums[i] + term
        values = [src[i, x] - sums[i] for i in range(nv)]
        for i in range(nv):
            res[i, x] = values[i]
        for i in range(nv):
            prov[i, x] = total([inv[i, j, x] * values[j] for j in range(nv)])
        return carry

    lax.fori_loop(0, planes, flux, 0)

    def residual_copy():
        return pltpu.make_async_copy(res, residual_out.at[0], out_sem.at[0])

    @pl.when(jnp.logical_not(stator_foot))
    def _():
        residual_copy().start()

    @pl.when(jnp.logical_not(has_low))
    def _():
        entering[...] = zero_plane

    @pl.when(jnp.logical_not(has_high))
    def _():
        following[...] = zero_plane

    @pl.when(stator_foot)
    def _():
        gather_facing(entering)

    def columns_of(k):
        return pl.ds(pl.multiple_of(k * GROUP, GROUP), GROUP)

    def forward_copy(k):
        return remote(
            prov.at[:, planes - 1, columns_of(k)], entering.at[:, columns_of(k)],
            fw_send.at[k], fw_recv.at[k], slab=slab + 1,
        )

    def backward_copy(k):
        return remote(
            upd.at[:, 0, columns_of(k)], following.at[:, columns_of(k)],
            bw_send.at[k], bw_recv.at[k], slab=slab - 1,
        )

    def forward(k, carry):
        @pl.when(has_low)
        def _():
            forward_copy(k).wait_recv()

        at = columns_of(k)
        now = [entering[v, at] for v in range(nv)]
        for x in range(planes):
            now = [
                total([prov[i, x, at]] + [eff[i, j, x, at] * now[j] for j in range(nv)])
                for i in range(nv)
            ]
            for i in range(nv):
                prov[i, x, at] = now[i]

        @pl.when(has_high)
        def _():
            forward_copy(k).start()

        return carry

    lax.fori_loop(0, groups, forward, 0)

    @pl.when(stator_foot)
    def _():
        ghost = [entering[v] for v in range(nv)]
        for i in range(nv):
            res[i, 0] = res[i, 0] + total(
                [(0.5 * axial[0, i, j]) * ghost[j] for j in range(nv)]
            )
        residual_copy().start()

    def state_copy(k):
        at = columns_of(k)
        return pltpu.make_async_copy(
            q.at[:, pl.ds(1, planes), pl.ds(pl.multiple_of(PAD + k * GROUP, GROUP), GROUP)],
            state_out.at[0, :, :, at], out_sem.at[1 + k],
        )

    def backward(k, carry):
        @pl.when(has_high)
        def _():
            backward_copy(k).wait_recv()

        at = columns_of(k)
        shifted = pl.ds(pl.multiple_of(PAD + k * GROUP, GROUP), GROUP)
        now = [following[v, at] for v in range(nv)]
        for x in reversed(range(planes)):
            now = [
                prov[i, x, at] - total([eff[i, j, x, at] * now[j] for j in range(nv)])
                for i in range(nv)
            ]
            if x == 0:
                for i in range(nv):
                    upd[i, 0, at] = now[i]

                @pl.when(has_low)
                def _():
                    backward_copy(k).start()

            for i in range(nv):
                q[i, x + 1, shifted] = q[i, x + 1, shifted] + now[i]
        state_copy(k).start()
        return carry

    to_after.wait_send()
    to_before.wait_send()

    @pl.when(has_high)
    def _():
        to_high.wait_send()

    @pl.when(has_low)
    def _():
        to_low.wait_send()

    @pl.when(on_plane)
    def _():
        for other in range(sectors):
            facing_copy(1, other).wait_send()

    lax.fori_loop(0, groups, backward, 0)

    def finish(k, carry):
        @pl.when(has_high)
        def _():
            forward_copy(k).wait_send()

        @pl.when(has_low)
        def _():
            backward_copy(k).wait_send()

        state_copy(k).wait()
        return carry

    lax.fori_loop(0, groups, finish, 0)
    residual_copy().wait()


def per_device(state, source, diag_inverse, jac_axial, jac_cross, owner):
    _, nv, planes, columns, cells = state.shape
    sectors = lax.axis_size("sector")
    slabs = lax.axis_size("slab")
    groups = columns // GROUP
    row = lax.axis_index("row")
    first = lax.axis_index("sector") * columns
    ids = first + jnp.arange(columns, dtype=jnp.int32)
    everyone = jnp.arange(owner.shape[0], dtype=jnp.int32)
    hits = jnp.where(
        row == 0, everyone[None, :] == ids[:, None], owner[None, :] == ids[:, None]
    )
    values = jnp.where(row == 0, owner, everyone)
    picks = jnp.sum(jnp.where(hits, values[None, :], 0), axis=1)

    def vmem(*shape):
        return pltpu.VMEM(shape, jnp.float32)

    dma = pltpu.SemaphoreType.DMA
    field = (nv, planes, columns, cells)
    plane = (nv, columns, cells)
    anywhere = pl.BlockSpec(memory_space=pl.ANY)
    scalars = pl.BlockSpec(memory_space=pltpu.SMEM)
    return pl.pallas_call(
        functools.partial(kernel, sectors, slabs),
        out_shape=[jax.ShapeDtypeStruct(state.shape, jnp.float32)] * 2,
        in_specs=[anywhere] * 3 + [scalars] * 3,
        out_specs=[anywhere] * 2,
        scratch_shapes=[
            vmem(nv, planes + 2, columns + 2 * PAD, cells),
            vmem(*field),
            vmem(nv, *field),
            vmem(nv, *field),
            vmem(*field),
            vmem(*field),
            vmem(nv, 1, columns, cells),
            vmem(sectors, *plane),
            vmem(*plane),
            vmem(*plane),
            dma((3,)), dma((1 + groups,)),
            dma((2,)), dma((2,)), dma((2,)), dma((2,)),
            dma((sectors,)), dma((sectors,)),
            dma((groups,)), dma((groups,)), dma((groups,)), dma((groups,)),
        ],
        compiler_params=pltpu.CompilerParams(collective_id=0, has_side_effects=True),
    )(state, source, diag_inverse, jac_axial, jac_cross, picks)


def solution(mesh):
    return jax.shard_map(
        per_device,
        mesh=mesh,
        in_specs=(
            P("row", None, "slab", "sector", None),
            P("row", None, "slab", "sector", None),
            P("row", None, None, "slab", "sector", None),
            P("row", None, None),
            P("row", None, None, None),
            P(),
        ),
        out_specs=(P("row", None, "slab", "sector", None), P("row", None, "slab", "sector", None)),
        check_vma=False,
    )
```

```python
import functools

import jax
import jax.numpy as jnp
from jax import lax
from jax.experimental import pallas as pl
from jax.experimental.pallas import tpu as pltpu
from jax.sharding import PartitionSpec as P

MESH = pl.DeviceIdType.MESH
PAD = 8
GROUP = 8


def total(terms):
    while len(terms) > 1:
        pairs = [a + b for a, b in zip(terms[::2], terms[1::2])]
        if len(terms) % 2:
            pairs.append(terms[-1])
        terms = pairs
    return terms[0]


def kernel(
    sectors, slabs,
    state, source, inverse, axial_in, cross_in, owner_in,
    res_out, state_out,
    axial, cross, owner, picks_wide, picks,
    q, src, inv, eff, prov, upd, facing, entering, following,
    local_sem, ax_send, ax_recv, se_send, se_recv,
    if_send, if_recv, fw_send, fw_recv, bw_send, bw_recv,
):
    nv, planes, columns, cells = src.shape
    groups = columns // GROUP
    row = lax.axis_index("row")
    sector = lax.axis_index("sector")
    slab = lax.axis_index("slab")
    has_low = slab > 0
    has_high = slab < slabs - 1
    rotor_top = jnp.logical_and(row == 0, slab == slabs - 1)
    stator_foot = jnp.logical_and(row == 1, slab == 0)
    on_plane = jnp.logical_or(rotor_top, stator_foot)
    after = lax.rem(sector + 1, sectors)
    before = lax.rem(sector + sectors - 1, sectors)
    facing_slab = jnp.where(row == 0, 0, slabs - 1)
    body = pl.ds(PAD, columns)

    load_state = pltpu.make_async_copy(
        state.at[0], q.at[:, pl.ds(1, planes), body], local_sem.at[0]
    )
    load_state.start()
    load_owner = pltpu.make_async_copy(owner_in, owner, local_sem.at[3])
    load_owner.start()
    load_axial = pltpu.make_async_copy(axial_in, axial, local_sem.at[4])
    load_axial.start()
    load_cross = pltpu.make_async_copy(cross_in, cross, local_sem.at[5])
    load_cross.start()
    load_inverse = pltpu.make_async_copy(inverse.at[0], inv, local_sem.at[2])
    load_inverse.start()
    load_source = pltpu.make_async_copy(source.at[0], src, local_sem.at[1])
    load_source.start()

    barrier = pltpu.get_barrier_semaphore()

    def greet(**where):
        pl.semaphore_signal(barrier, inc=1, device_id=where, device_id_type=MESH)

    @pl.when(on_plane)
    def _():
        for other in range(sectors):
            greet(row=1 - row, sector=other, slab=facing_slab)

    greet(sector=after)
    greet(sector=before)

    @pl.when(has_low)
    def _():
        greet(slab=slab - 1)

    @pl.when(has_high)
    def _():
        greet(slab=slab + 1)

    zero_plane = jnp.zeros((nv, columns, cells), jnp.float32)

    @pl.when(jnp.logical_not(has_low))
    def _():
        q[:, 0, body] = zero_plane

    @pl.when(jnp.logical_not(has_high))
    def _():
        q[:, planes + 1, body] = zero_plane

    load_owner.wait()
    shape = (columns, owner.shape[1])
    ids = sector * columns + lax.broadcasted_iota(jnp.int32, shape, 0)
    everyone = lax.broadcasted_iota(jnp.int32, shape, 1)
    owners = jnp.broadcast_to(owner[...], shape)
    is_rotor = jnp.broadcast_to(row, shape) == 0
    hits = jnp.where(is_rotor, everyone, owners) == ids
    found = jnp.sum(
        jnp.where(hits, jnp.where(is_rotor, owners, everyone), 0), axis=1, keepdims=True
    )
    found = jnp.minimum(found, owner.shape[1] - 1)
    picks_wide[...] = jnp.broadcast_to(found, picks_wide.shape)
    move_picks = pltpu.make_async_copy(picks_wide, picks, local_sem.at[6])
    move_picks.start()
    peers = 2 + has_low.astype(jnp.int32) + has_high.astype(jnp.int32)
    pl.semaphore_wait(barrier, peers + jnp.where(on_plane, sectors, 0))

    load_state.wait()

    def remote(source_ref, target_ref, send, recv, **where):
        return pltpu.make_async_remote_copy(
            src_ref=source_ref, dst_ref=target_ref, send_sem=send, recv_sem=recv,
            device_id=where, device_id_type=MESH,
        )

    def facing_copy(plane_at, other):
        return remote(
            q.at[:, plane_at, body], facing.at[sector], if_send.at[other], if_recv.at[sector],
            row=1 - row, sector=other, slab=facing_slab,
        )

    def facing_arrival(other):
        return remote(
            q.at[:, 1, body], facing.at[other], if_send.at[other], if_recv.at[other],
            row=1 - row, sector=other, slab=facing_slab,
        )

    @pl.when(rotor_top)
    def _():
        for other in range(sectors):
            facing_copy(planes, other).start()

    @pl.when(stator_foot)
    def _():
        for other in range(sectors):
            facing_copy(1, other).start()

    inner = pl.ds(1, planes)
    to_after = remote(
        q.at[:, inner, pl.ds(PAD + columns - 1, 1)], q.at[:, inner, pl.ds(PAD - 1, 1)],
        se_send.at[0], se_recv.at[0], sector=after,
    )
    to_before = remote(
        q.at[:, inner, pl.ds(PAD, 1)], q.at[:, inner, pl.ds(PAD + columns, 1)],
        se_send.at[1], se_recv.at[1], sector=before,
    )
    to_after.start()
    to_before.start()
    to_high = remote(
        q.at[:, planes, body], q.at[:, 0, body], ax_send.at[0], ax_recv.at[0], slab=slab + 1
    )
    to_low = remote(
        q.at[:, 1, body], q.at[:, planes + 1, body], ax_send.at[1], ax_recv.at[1], slab=slab - 1
    )

    @pl.when(has_high)
    def _():
        to_high.start()

    @pl.when(has_low)
    def _():
        to_low.start()

    load_inverse.wait()
    load_axial.wait()
    load_cross.wait()
    move_picks.wait()

    def effective(x, carry):
        for i in range(nv):
            blocks = [inv[i, j, x] for j in range(nv)]
            for k in range(nv):
                eff[i, k, x] = total([blocks[j] * (0.5 * axial[j, 0, k]) for j in range(nv)])
        return carry

    lax.fori_loop(0, planes, effective, 0)
    load_source.wait()
    to_after.wait_recv()
    to_before.wait_recv()

    @pl.when(has_high)
    def _():
        to_low.wait_recv()

    @pl.when(has_low)
    def _():
        to_high.wait_recv()

    def gather_facing(target):
        for other in range(sectors):
            facing_arrival(other).wait_recv()

        def pick(c, carry):
            at = picks[c, 0]
            part, column = at // columns, lax.rem(at, columns)
            for v in range(nv):
                target[v, pl.ds(c, 1)] = facing[part, v, pl.ds(column, 1)]
            return carry

        lax.fori_loop(0, columns, pick, 0)

    @pl.when(rotor_top)
    def _():
        gather_facing(q.at[:, planes + 1, body])

    lane = lax.broadcasted_iota(jnp.int32, (columns, cells), 1)

    def flux(x, carry):
        sums = [None] * nv
        for v in range(nv):
            here = q[v, x + 1, body]
            spans = (
                q[v, x + 2, body] - q[v, x, body],
                q[v, x + 1, pl.ds(PAD + 1, columns)] - q[v, x + 1, pl.ds(PAD - 1, columns)],
                jnp.where(lane == cells - 1, 0.0, pltpu.roll(here, cells - 1, 1))
                - jnp.where(lane == 0, 0.0, pltpu.roll(here, 1, 1)),
            )
            for i in range(nv):
                factors = (axial[i, 0, v], cross[0, i, 0, v], cross[0, i, 1, v])
                term = total([(0.5 * f) * s for f, s in zip(factors, spans)])
                sums[i] = term if sums[i] is None else sums[i] + term
        values = [src[i, x] - sums[i] for i in range(nv)]
        for i in range(nv):
            res_out[0, i, x] = values[i]
        for i in range(nv):
            prov[i, x] = total([inv[i, j, x] * values[j] for j in range(nv)])
        return carry

    lax.fori_loop(0, planes, flux, 0)

    @pl.when(jnp.logical_not(has_low))
    def _():
        entering[...] = zero_plane

    @pl.when(jnp.logical_not(has_high))
    def _():
        following[...] = zero_plane

    @pl.when(stator_foot)
    def _():
        gather_facing(entering)

    def columns_of(k):
        return pl.ds(pl.multiple_of(k * GROUP, GROUP), GROUP)

    def forward_copy(k):
        return remote(
            prov.at[:, planes - 1, columns_of(k)], entering.at[:, columns_of(k)],
            fw_send.at[k], fw_recv.at[k], slab=slab + 1,
        )

    def backward_copy(k):
        return remote(
            upd.at[:, 0, columns_of(k)], following.at[:, columns_of(k)],
            bw_send.at[k], bw_recv.at[k], slab=slab - 1,
        )

    def forward(k, carry):
        @pl.when(has_low)
        def _():
            forward_copy(k).wait_recv()

        at = columns_of(k)
        now = [entering[v, at] for v in range(nv)]
        for x in range(planes):
            now = [
                total([prov[i, x, at]] + [eff[i, j, x, at] * now[j] for j in range(nv)])
                for i in range(nv)
            ]
            for i in range(nv):
                prov[i, x, at] = now[i]

        @pl.when(has_high)
        def _():
            forward_copy(k).start()

        return carry

    lax.fori_loop(0, groups, forward, 0)

    @pl.when(stator_foot)
    def _():
        ghost = [entering[v] for v in range(nv)]
        for i in range(nv):
            res_out[0, i, 0] = res_out[0, i, 0] + total(
                [(0.5 * axial[i, 0, j]) * ghost[j] for j in range(nv)]
            )

    def backward(k, carry):
        @pl.when(has_high)
        def _():
            backward_copy(k).wait_recv()

        at = columns_of(k)
        shifted = pl.ds(pl.multiple_of(PAD + k * GROUP, GROUP), GROUP)
        now = [following[v, at] for v in range(nv)]
        for x in reversed(range(planes)):
            now = [
                prov[i, x, at] - total([eff[i, j, x, at] * now[j] for j in range(nv)])
                for i in range(nv)
            ]
            if x == 0:
                for i in range(nv):
                    upd[i, 0, at] = now[i]

                @pl.when(has_low)
                def _():
                    backward_copy(k).start()

            for i in range(nv):
                state_out[0, i, x, at] = q[i, x + 1, shifted] + now[i]
        return carry

    to_after.wait_send()
    to_before.wait_send()

    @pl.when(has_high)
    def _():
        to_high.wait_send()

    @pl.when(has_low)
    def _():
        to_low.wait_send()

    @pl.when(on_plane)
    def _():
        for other in range(sectors):
            facing_copy(1, other).wait_send()

    lax.fori_loop(0, groups, backward, 0)

    def finish(k, carry):
        @pl.when(has_high)
        def _():
            forward_copy(k).wait_send()

        @pl.when(has_low)
        def _():
            backward_copy(k).wait_send()

        return carry

    lax.fori_loop(0, groups, finish, 0)


def per_device(state, source, diag_inverse, jac_axial, jac_cross, owner):
    _, nv, planes, columns, cells = state.shape
    sectors = lax.axis_size("sector")
    slabs = lax.axis_size("slab")
    groups = columns // GROUP
    def vmem(*shape):
        return pltpu.VMEM(shape, jnp.float32)

    dma = pltpu.SemaphoreType.DMA
    field = (nv, planes, columns, cells)
    plane = (nv, columns, cells)
    anywhere = pl.BlockSpec(memory_space=pl.ANY)
    outside = pl.BlockSpec(memory_space=pltpu.HBM)
    return pl.pallas_call(
        functools.partial(kernel, sectors, slabs),
        out_shape=[vmem(*state.shape)] * 2,
        in_specs=[outside] * 6,
        out_specs=[pl.BlockSpec(memory_space=pltpu.VMEM)] * 2,
        scratch_shapes=[
            pltpu.SMEM((nv, 1, nv), jnp.float32),
            pltpu.SMEM((1, nv, 2, nv), jnp.float32),
            pltpu.VMEM((1, owner.shape[0]), jnp.int32),
            pltpu.VMEM((columns, 128), jnp.int32),
            pltpu.SMEM((columns, 128), jnp.int32),
            vmem(nv, planes + 2, columns + 2 * PAD, cells),
            vmem(*field),
            vmem(nv, *field),
            vmem(nv, *field),
            vmem(*field),
            vmem(nv, 1, columns, cells),
            vmem(sectors, *plane),
            vmem(*plane),
            vmem(*plane),
            dma((7,)),
            dma((2,)), dma((2,)), dma((2,)), dma((2,)),
            dma((sectors,)), dma((sectors,)),
            dma((groups,)), dma((groups,)), dma((groups,)), dma((groups,)),
        ],
        compiler_params=pltpu.CompilerParams(collective_id=0, has_side_effects=True),
    )(state, source, diag_inverse, jnp.swapaxes(jac_axial, 0, 1),
        jnp.swapaxes(jac_cross, 1, 2), owner[None])


def solution(mesh):
    return jax.shard_map(
        per_device,
        mesh=mesh,
        in_specs=(
            P("row", None, "slab", "sector", None),
            P("row", None, "slab", "sector", None),
            P("row", None, None, "slab", "sector", None),
            P("row", None, None),
            P("row", None, None, None),
            P(),
        ),
        out_specs=(P("row", None, "slab", "sector", None), P("row", None, "slab", "sector", None)),
        check_vma=False,
    )
```
